32 devices in a mesh: grp: 2 (over y), ep: 16 (over z, x, core), sess: 1.
Axes of the slice: x: 2, y: 2, z: 4, core: 2. Of those that a mesh axis runs over, the one named last changes fastest.
Arguments:
- thinker_rows: bfloat16 [1024, 2048], P(('grp', 'ep', 'sess')), parts along dimension 0, may hold values from -6 to 6
- think_route: int32 [1024, 8], P(('grp', 'ep', 'sess')), parts along dimension 0, may hold values from 0 to 15, all different within a row; in each aligned block of 32 rows (0 to 31, 32 to 63, ...) at most 32 rows name the same one
- think_weight: float32 [1024, 8], P(('grp', 'ep', 'sess')), parts along dimension 0, may hold values from 0.1 to 1
- think_gate: bfloat16 [16, 2048, 768], P('ep', None, 'sess'), may hold values from -0.125 to 0.125
- think_up: bfloat16 [16, 2048, 768], P('ep', None, 'sess'), may hold values from -0.125 to 0.125
- think_down: bfloat16 [16, 768, 2048], P('ep', 'sess'), may hold values from -0.21875 to 0.21875
- proj_weight: bfloat16 [2048, 1024], P(None, 'sess'), may hold values from -0.125 to 0.125
- owner_map: int32 [1024], P(('grp', 'ep')), parts along dimension 0, may hold values from 0 to 31, as said below
- talk_gain: float32 [1024], replicated, may hold values from 0.5 to 1.5
- talk_route: int32 [1024, 6], P(('grp', 'ep', 'sess')), parts along dimension 0, may hold values from 0 to 15, all different within a row; in each aligned block of 32 rows (0 to 31, 32 to 63, ...) at most 24 rows name the same one
- talk_weight: float32 [1024, 6], P(('grp', 'ep', 'sess')), parts along dimension 0, may hold values from 0.1 to 1
- talk_gate: bfloat16 [16, 1024, 384], P(('ep', 'sess')), may hold values from -0.1875 to 0.1875
- talk_up: bfloat16 [16, 1024, 384], P(('ep', 'sess')), may hold values from -0.1875 to 0.1875
- talk_down: bfloat16 [16, 384, 1024], P(('ep', 'sess')), may hold values from -0.3125 to 0.3125
Outputs:
- thinker_branch: bfloat16 [1024, 2048], P(('grp', 'ep', 'sess')), parts along dimension 0
- talker_branch: bfloat16 [1024, 1024], P(('grp', 'ep', 'sess')), parts along dimension 0
The draws below stay inside these ranges and needn't reach their ends.
There are 2 independent parts, one for each index of `grp`. The reference program is written for one: setup_inputs(seed, part) draws one part's arguments, and reference() takes and returns one part's arrays. A program takes and returns all parts, laid end to end along the dimension named above; an argument that names none is the same for every part. Nothing has to cross between parts.
Inputs may be any that keep to these rules, and one draw needn't show every extreme that they name: `think_route`: within each aligned block of 32 rows (the rows of one device) no thinker expert is named by more than 32 rows, a bound that some block reaches. `talk_route`: within each aligned block of 32 rows (the rows of one device) no talker expert is named by more than 24 rows, a bound that some block reaches. `owner_map`: each aligned block of 32 entries holds every value of its range exactly once.
All inputs are finite; a program needn't handle non-finite values.
Results may differ from the reference program's by a relative error of at most 0.015.
Values may be sent and summed in bfloat16 or wider, within the bound.
No kernel may reach another device: no remote copies, remote signals or barrier semaphores. Data moves between devices by JAX's collectives and lax.ppermute only.
A program may use at most 64 MiB of HBM per device.

```python
import math
import jax
import jax.numpy as jnp
import numpy as np
from jax import lax

D = 2048
FF_T = 768
TW = 1024
FF_K = 384
TOP_T = 8
TOP_K = 6
ROWS_DEV = 32
SESSIONS = 512
PAIR_ROWS = 32
EXPERTS_T = 16
EXPERTS_K = 16
CAP_T = 32
CAP_K = 24


def draw_owner_map(key, part):
    block_rows = PAIR_ROWS
    blocks = SESSIONS // block_rows
    keys = jax.random.split(jax.random.fold_in(key, 7), blocks)
    orders = jax.vmap(lambda single: jax.random.permutation(single, block_rows))(keys)
    return orders.reshape(SESSIONS).astype(jnp.int32)


def block_scale(key, shape, cuts, low, high):
    factor_of, own = 1.0, jax.random.fold_in(key, 6)
    for position, blocks in cuts:
        heights = jnp.exp(jax.random.uniform(jax.random.fold_in(own, position), (blocks,), jnp.float32, low / len(cuts), high / len(cuts)))
        factor_of = factor_of * jnp.repeat(heights, shape[position] // blocks).reshape([-1 if axis == position else 1 for axis in range(len(shape))])
    return factor_of


def assign_block(key, own, number, rows, number_of, top, bound, lean):
    sequence = jax.random.permutation(key, number_of)
    crowded, ordinary = shares(number_of, rows * top, bound, lean, True), shares(number_of, rows * top, bound, lean, False)
    places = jnp.arange(number_of)

    def named(lengths, turn):
        used = int((lengths > 0).sum())
        fixed = max(1, used // 4)
        moved = fixed + (places - fixed + turn * (used - fixed)) % max(1, number_of - fixed)
        return jnp.zeros((number_of,), jnp.int32).at[sequence[jnp.where(places < fixed, places, moved)]].set(jnp.asarray(lengths, jnp.int32))

    lengths = jnp.where(number % 4 == 0, named(crowded, number // 4), named(ordinary, number - number // 4 - 1))
    mixed = jax.random.permutation(jax.random.fold_in(own, 3), number_of)
    source_of, receiver = mixed[0:number_of // 2 * 2:2], mixed[1:number_of // 2 * 2:2]
    margin = jnp.minimum(lengths[source_of] - 1, bound - lengths[receiver]) // 2
    margin = jnp.where((source_of == sequence[0]) | (receiver == sequence[0]) | (lengths[receiver] == 0), 0, jnp.maximum(margin, 0))
    moved = jax.random.randint(jax.random.fold_in(own, 4), (number_of // 2,), 0, 1 << 20) % (margin + 1)
    lengths = lengths.at[source_of].add(-moved).at[receiver].add(moved)
    members = jnp.searchsorted(jnp.cumsum(lengths), jnp.arange(rows * top), side="right").astype(jnp.int32)
    grid = members.reshape(top, rows).T
    grid = grid[jax.random.permutation(jax.random.fold_in(own, 1), rows)]
    turn = jax.random.randint(jax.random.fold_in(own, 2), (rows, 1), 0, top)
    return jnp.take_along_axis(grid, (jnp.arange(top)[None, :] + turn) % top, axis=1)


def shares(number_of, total, reach, lean, full):
    loads = [(1 << 20) // math.isqrt(standing ** lean) + 1 for standing in range(1, number_of + 1)]
    largest = reach if full else min(reach, max(-(-total // number_of), total * loads[0] // sum(loads)))
    least = 1 if total - largest >= number_of - 1 else 0
    counts, spare = [largest] + [least] * (number_of - 1), total - largest - least * (number_of - 1)
    while spare > 0:
        candidates = [i for i in range(1, number_of) if counts[i] < largest] or [i for i in range(1, number_of) if counts[i] < reach]
        whole, left = sum([loads[i] for i in candidates]), spare
        for i in candidates:
            extra = min(reach - counts[i], max(1, left * loads[i] // whole), spare)
            counts[i] = counts[i] + extra
            spare = spare - extra
    return np.array(counts)


def centred(own_key, extent, width, bound, shards=(), held_as=jnp.bfloat16):
    level = block_scale(own_key, extent, shards, -0.22, 0.18) if shards else 1.0
    drawn = jax.random.normal(own_key, extent, jnp.float32) * width * level
    return jnp.minimum(jnp.maximum(drawn, -bound), bound).astype(held_as)


def setup_inputs(seed: int = 0, part: int = 0) -> dict:
    key_list = jax.random.split(jax.random.key(seed), 15)
    own_keys = jax.random.split(jax.random.fold_in(key_list[14], part), 15)
    thinker_rows = centred(own_keys[0], (SESSIONS, D), 1.0, 6.0, ((0, 16),))
    think_route_keys = jax.random.split(jax.random.fold_in(own_keys[1], 1), SESSIONS // ROWS_DEV)
    think_route_turns = jax.random.permutation(jax.random.fold_in(own_keys[1], 3), SESSIONS // ROWS_DEV)
    think_route = jax.vmap(lambda own, number: assign_block(jax.random.fold_in(own_keys[1], 2), own, number, ROWS_DEV, EXPERTS_T, TOP_T, CAP_T, 2))(think_route_keys, think_route_turns).reshape((SESSIONS, TOP_T))
    think_weight = jnp.clip(jnp.exp(math.log(1.0) - 2.3025851 * jax.random.uniform(own_keys[2], (SESSIONS, TOP_T), jnp.float32) ** block_scale(own_keys[2], (SESSIONS, TOP_T), ((0, 16),), -0.2, 0.2)), 0.1, 1.0)
    think_gate = centred(key_list[3], (EXPERTS_T, D, FF_T), D ** -0.5, 0.125, ((0, 16),))
    think_up = centred(key_list[4], (EXPERTS_T, D, FF_T), D ** -0.5, 0.125, ((0, 16),))
    think_down = centred(key_list[5], (EXPERTS_T, FF_T, D), FF_T ** -0.5, 0.21875, ((0, 16),))
    proj_weight = centred(key_list[6], (D, TW), D ** -0.5, 0.125)
    owner_map = draw_owner_map(jax.random.fold_in(jax.random.fold_in(key_list[14], part), 71), part)
    talk_gain = jnp.clip(1.0 + 0.1 * jax.random.normal(key_list[8], (TW,), jnp.float32), 0.5, 1.5)
    talk_route_keys = jax.random.split(jax.random.fold_in(own_keys[9], 1), SESSIONS // ROWS_DEV)
    talk_route_turns = jax.random.permutation(jax.random.fold_in(own_keys[9], 3), SESSIONS // ROWS_DEV)
    talk_route = jax.vmap(lambda own, number: assign_block(jax.random.fold_in(own_keys[9], 2), own, number, ROWS_DEV, EXPERTS_K, TOP_K, CAP_K, 2))(talk_route_keys, talk_route_turns).reshape((SESSIONS, TOP_K))
    talk_weight = jnp.clip(jnp.exp(math.log(1.0) - 2.3025851 * jax.random.uniform(own_keys[10], (SESSIONS, TOP_K), jnp.float32) ** block_scale(own_keys[10], (SESSIONS, TOP_K), ((0, 16),), -0.2, 0.2)), 0.1, 1.0)
    talk_gate = centred(key_list[11], (EXPERTS_K, TW, FF_K), TW ** -0.5, 0.1875, ((0, 16),))
    talk_up = centred(key_list[12], (EXPERTS_K, TW, FF_K), TW ** -0.5, 0.1875, ((0, 16),))
    talk_down = centred(key_list[13], (EXPERTS_K, FF_K, TW), FF_K ** -0.5, 0.3125, ((0, 16),))
    return {"thinker_rows": thinker_rows, "think_route": think_route, "think_weight": think_weight, "think_gate": think_gate, "think_up": think_up, "think_down": think_down, "proj_weight": proj_weight, "owner_map": owner_map, "talk_gain": talk_gain, "talk_route": talk_route, "talk_weight": talk_weight, "talk_gate": talk_gate, "talk_up": talk_up, "talk_down": talk_down}


def slot_places(route, rows_per, experts):
    sessions, picks = route.shape
    blocks = sessions // rows_per
    grouped = route.reshape(blocks, rows_per * picks)
    onehot = (grouped[:, :, None] == jnp.arange(experts, dtype=jnp.int32)[None, None, :]).astype(jnp.int32)
    before = jnp.cumsum(onehot, axis=1) - onehot
    return lax.optimization_barrier(jnp.sum(before * onehot, axis=2)).reshape(sessions * picks).astype(jnp.int32)

def mixture(row_block, route, weights, gate_w, up_w, down_w, rows_per, capacity):
    sessions, picks = route.shape
    experts = gate_w.shape[0]
    features = row_block.shape[1]
    blocks = sessions // rows_per
    places = slot_places(route, rows_per, experts)
    chosen = route.reshape(sessions * picks).astype(jnp.int32)
    owner_block = (jnp.arange(sessions * picks, dtype=jnp.int32) // (rows_per * picks)).astype(jnp.int32)
    target = chosen * (blocks * capacity) + owner_block * capacity + places
    copies = jnp.repeat(row_block, picks, axis=0)
    buffer = jnp.zeros((experts * blocks * capacity, features), row_block.dtype).at[target].set(copies)
    buffer = buffer.reshape(experts, blocks * capacity, features)

    def one_expert(operands):
        slab, gate_m, up_m, down_m = operands
        gate = jnp.dot(slab, gate_m, preferred_element_type=jnp.float32)
        upper = jnp.dot(slab, up_m, preferred_element_type=jnp.float32)
        hidden = (jax.nn.silu(gate) * upper).astype(jnp.bfloat16)
        return jnp.dot(hidden, down_m, preferred_element_type=jnp.float32).astype(jnp.bfloat16)
    outputs = lax.map(one_expert, (buffer, gate_w, up_w, down_w)).reshape(experts * blocks * capacity, features)
    gathered = outputs[target].astype(jnp.float32).reshape(sessions, picks, features)
    norm_weights = weights / lax.optimization_barrier(jnp.sum(weights, axis=1, keepdims=True))
    return lax.optimization_barrier(jnp.sum(gathered * norm_weights[:, :, None], axis=1)).astype(jnp.bfloat16)

def reference(thinker_rows, think_route, think_weight, think_gate, think_up, think_down, proj_weight, owner_map, talk_gain, talk_route, talk_weight, talk_gate, talk_up, talk_down):
    thinker_branch = mixture(thinker_rows, think_route, think_weight, think_gate, think_up, think_down, ROWS_DEV, CAP_T)
    projected = jnp.dot(thinker_branch, proj_weight, preferred_element_type=jnp.float32).astype(jnp.bfloat16)
    block_rows = PAIR_ROWS
    source = jnp.arange(SESSIONS, dtype=jnp.int32) // block_rows * block_rows + owner_map.astype(jnp.int32)
    relayed = projected[source].astype(jnp.float32)
    scale = lax.rsqrt(lax.optimization_barrier(jnp.mean(relayed * relayed, axis=1, keepdims=True)) + 1e-06)
    talk_rows = (relayed * scale * talk_gain[None, :]).astype(jnp.bfloat16)
    talker_branch = mixture(talk_rows, talk_route, talk_weight, talk_gate, talk_up, talk_down, ROWS_DEV, CAP_K)
    return (thinker_branch, talker_branch)
```

```python
import functools

import jax
import jax.numpy as jnp
from jax import lax
from jax.experimental import pallas as pl
from jax.experimental.pallas import tpu as pltpu
from jax.sharding import PartitionSpec as P


def slot_places(route, experts):
    picks = route.shape[0] * route.shape[1]
    chosen = route.reshape(picks)
    onehot = (chosen[:, None] == jnp.arange(experts, dtype=jnp.int32)[None, :]).astype(jnp.int32)
    before = jnp.cumsum(onehot, axis=0) - onehot
    return (chosen, jnp.sum(before * onehot, axis=1))


def pack_rows(row_block, route, experts, capacity):
    chosen, places = slot_places(route, experts)
    target = chosen * capacity + places
    copies = jnp.repeat(row_block, route.shape[1], axis=0)
    buffer = (
        jnp.zeros((experts * capacity, row_block.shape[1]), jnp.bfloat16).at[target].set(copies)
    )
    return (buffer, target)


def combine_rows(returned, target, weights):
    sessions, picks = weights.shape
    gathered = returned[target].astype(jnp.float32).reshape(sessions, picks, returned.shape[1])
    norm_weights = weights / jnp.sum(weights, axis=1, keepdims=True)
    return jnp.sum(gathered * norm_weights[:, :, None], axis=1).astype(jnp.bfloat16)


def swiglu(slab, gate_m, up_m, down_m):
    gate = jnp.dot(slab, gate_m, preferred_element_type=jnp.float32)
    upper = jnp.dot(slab, up_m, preferred_element_type=jnp.float32)
    hidden = (jax.nn.silu(gate) * upper).astype(jnp.bfloat16)
    return jnp.dot(hidden, down_m, preferred_element_type=jnp.float32)


def on_device(
    thinker_rows,
    think_route,
    think_weight,
    think_gate,
    think_up,
    think_down,
    proj_weight,
    owner_map,
    talk_gain,
    talk_route,
    talk_weight,
    talk_gate,
    talk_up,
    talk_down,
):
    sessions = thinker_rows.shape[0]
    features = thinker_rows.shape[1]
    talk_features = talk_gate.shape[1]
    ep_count = lax.axis_size("ep")
    sess_count = lax.axis_size("sess")
    think_picks = think_route.shape[1]
    think_capacity = min(sessions, max(2, 2 * sessions * think_picks // ep_count))
    buffer, target = pack_rows(thinker_rows, think_route, ep_count, think_capacity)
    buffer = buffer.reshape(ep_count, think_capacity, features)
    gate_half = think_gate[0]
    up_half = think_up[0]
    down_half = think_down[0]
    paired = lax.all_gather(buffer, "sess", axis=1, tiled=True)
    arrived = lax.all_to_all(paired, "ep", split_axis=0, concat_axis=0, tiled=True)
    flattened = arrived.reshape(arrived.shape[0] * arrived.shape[1], features)
    result = swiglu(flattened, gate_half, up_half, down_half)
    partial_value = result.reshape(arrived.shape[0], arrived.shape[1], features)
    summed = lax.psum_scatter(partial_value, "sess", scatter_dimension=1, tiled=True).astype(
        jnp.bfloat16
    )
    returned = lax.all_to_all(summed, "ep", split_axis=0, concat_axis=0, tiled=True).reshape(
        ep_count * think_capacity, features
    )
    thinker_branch = combine_rows(returned, target, think_weight)
    projected = jnp.dot(
        lax.all_gather(thinker_branch, "sess", axis=0, tiled=True),
        proj_weight,
        preferred_element_type=jnp.float32,
    ).astype(jnp.bfloat16)
    block_rows = owner_map.shape[0]
    picker = (owner_map[:, None] == jnp.arange(block_rows, dtype=jnp.int32)[None, :]).astype(
        jnp.bfloat16
    )
    selected = jnp.dot(picker, projected, preferred_element_type=jnp.float32).astype(jnp.bfloat16)
    own_rows = lax.all_to_all(selected, "sess", split_axis=0, concat_axis=1, tiled=True).astype(
        jnp.float32
    )
    scale = lax.rsqrt(jnp.mean(own_rows * own_rows, axis=1, keepdims=True) + 1e-06)
    talk_rows = (own_rows * scale * talk_gain[None, :]).astype(jnp.bfloat16)
    talk_experts = ep_count * sess_count
    talk_picks = talk_route.shape[1]
    talk_capacity = min(sessions, max(2, 2 * sessions * talk_picks // talk_experts))
    talk_buffer, talk_target = pack_rows(talk_rows, talk_route, talk_experts, talk_capacity)
    talk_gate_m = talk_gate[0]
    talk_up_m = talk_up[0]
    talk_down_m = talk_down[0]
    sectioned_in = talk_buffer.reshape(talk_experts, talk_capacity, talk_features)
    portion = lax.all_to_all(sectioned_in, ("ep", "sess"), split_axis=0, concat_axis=0, tiled=True)
    flattened = portion.reshape(portion.shape[0] * portion.shape[1], talk_features)
    result = swiglu(flattened, talk_gate_m, talk_up_m, talk_down_m).astype(jnp.bfloat16)
    finished = result.reshape(portion.shape[0], portion.shape[1], talk_features)
    talk_returned = lax.all_to_all(
        finished, ("ep", "sess"), split_axis=0, concat_axis=0, tiled=True
    )
    talk_returned = talk_returned.reshape(talk_experts * talk_capacity, talk_features)
    talker_branch = combine_rows(talk_returned, talk_target, talk_weight)
    return (thinker_branch, talker_branch)


VMEM = pl.BlockSpec(memory_space=pltpu.VMEM)
SMEM = pl.BlockSpec(memory_space=pltpu.SMEM)
LANES = 128


def width_of_table(experts):
    return -(-4 * experts // LANES) * LANES


def share_table(lane, route_ref, weight_ref, first, experts):
    weights = weight_ref[...]
    shares = weights / jnp.sum(weights, axis=1, keepdims=True)
    table = jnp.zeros(lane.shape, jnp.float32)
    for pick in range(weights.shape[1]):
        expert = route_ref[:, pick : pick + 1] + first
        hit = (lane == expert) | (lane == expert + experts)
        table = table + jnp.where(hit, shares[:, pick : pick + 1], 0.0)
    return table


def pack_kernel(experts, rows_ref, route_ref, weight_ref, talk_route_ref, talk_weight_ref, out_ref):
    count, features = rows_ref.shape
    out_ref[:, :features] = rows_ref[...]
    lane = lax.broadcasted_iota(jnp.int32, (count, out_ref.shape[1] - features), 1)
    table = share_table(lane, route_ref, weight_ref, 0, experts)
    table = table + share_table(lane, talk_route_ref, talk_weight_ref, 2 * experts, experts)
    high = table.astype(jnp.bfloat16).astype(jnp.float32)
    fine = ((lane >= experts) & (lane < 2 * experts)) | (lane >= 3 * experts)
    out_ref[:, features:] = jnp.where(fine, table - high, high).astype(jnp.bfloat16)


def pack(rows, route, weight, talk_route, talk_weight, experts):
    count, features = rows.shape
    return pl.pallas_call(
        functools.partial(pack_kernel, experts),
        out_shape=jax.ShapeDtypeStruct((count, features + width_of_table(experts)), jnp.bfloat16),
        in_specs=[VMEM] * 5,
        out_specs=VMEM,
        compiler_params=pltpu.CompilerParams(vmem_limit_bytes=8 << 20),
        cost_estimate=pl.CostEstimate(flops=1 << 20, bytes_accessed=1 << 18, transcendentals=0),
        name="pack",
    )(rows, route, weight, talk_route, talk_weight)


def share_of(columns, first, experts, expert):
    lane = lax.broadcasted_iota(jnp.int32, columns.shape, 1)
    hit = (lane == first + expert) | (lane == first + experts + expert)
    return jnp.sum(jnp.where(hit, columns.astype(jnp.float32), 0.0), axis=1, keepdims=True)


def tile_of(width, most):
    tile = min(width, most)
    while width % tile:
        tile -= LANES
    return tile


def experts_of_block(slab_ref, hidden_ref, share, gate_ref, up_ref, down_ref, put):
    slab = slab_ref[...]
    hidden_units = gate_ref.shape[-1]
    step = tile_of(hidden_units, 256)
    for start in range(0, hidden_units, step):
        cut = slice(start, start + step)
        gate = jnp.dot(slab, gate_ref[0, :, cut], preferred_element_type=jnp.float32)
        upper = jnp.dot(slab, up_ref[0, :, cut], preferred_element_type=jnp.float32)
        hidden = gate / (1.0 + jnp.exp(-gate)) * upper
        hidden_ref[:, cut] = (hidden * share).astype(jnp.bfloat16)
    hidden = hidden_ref[...]
    features = down_ref.shape[-1]
    step = tile_of(features, 512)
    for start in range(0, features, step):
        cut = slice(start, start + step)
        put(cut, jnp.dot(hidden, down_ref[0, :, cut], preferred_element_type=jnp.float32))


def expert_kernel(count, groups, experts, first, expert_ref, *refs):
    blocks = refs[:count]
    tables = refs[count : 2 * count]
    gate_ref, up_ref, down_ref = refs[2 * count : 2 * count + 3]
    outs = refs[2 * count + 3 : -2]
    slab_ref, hidden_ref = refs[-2:]
    rows = blocks[0].shape[0]
    features = slab_ref.shape[1]
    shares = []
    for index, (block, table) in enumerate(zip(blocks, tables, strict=True)):
        slab_ref[index * rows : (index + 1) * rows, :] = block[:, :features]
        columns = table[:, table.shape[1] - width_of_table(experts) :]
        shares.append(share_of(columns, first, experts, expert_ref[0]))
    share = jnp.concatenate(shares, axis=0)

    def put(cut, value):
        value = value.astype(jnp.bfloat16)
        for out, group in zip(outs, groups, strict=True):
            for place, index in enumerate(group):
                out[place * rows : (place + 1) * rows, cut] = value[index * rows : (index + 1) * rows]

    experts_of_block(slab_ref, hidden_ref, share, gate_ref, up_ref, down_ref, put)


def run_expert(blocks, tables, groups, gate, up, down, expert, experts, first, name):
    count, rows = len(blocks), blocks[0].shape[0]
    _, features, hidden_units = gate.shape
    total = count * rows
    limit = 4 * total * features + 4 * total * hidden_units + (16 << 20)
    return pl.pallas_call(
        functools.partial(expert_kernel, count, groups, experts, first),
        out_shape=[jax.ShapeDtypeStruct((len(g) * rows, features), jnp.bfloat16) for g in groups],
        in_specs=[SMEM] + [VMEM] * (2 * count + 3),
        out_specs=[VMEM] * len(groups),
        scratch_shapes=[
            pltpu.VMEM((total, features), jnp.bfloat16),
            pltpu.VMEM((total, hidden_units), jnp.bfloat16),
        ],
        compiler_params=pltpu.CompilerParams(vmem_limit_bytes=limit),
        cost_estimate=pl.CostEstimate(
            flops=6 * total * features * hidden_units,
            bytes_accessed=6 * features * hidden_units,
            transcendentals=total * hidden_units,
        ),
        name=name,
    )(expert, *blocks, *tables, gate, up, down)


def relay_kernel(count, *refs):
    parts = refs[:count]
    proj_ref, owner_ref, gain_ref, branch_ref, rows_ref = refs[count:]
    rows = branch_ref.shape[0]
    total = parts[0][...].astype(jnp.float32)[:rows]
    for part in parts[1:]:
        total = total + part[...].astype(jnp.float32)[:rows]
    branch = total.astype(jnp.bfloat16)
    branch_ref[...] = branch
    source = lax.broadcasted_iota(jnp.int32, (rows, rows), 1)
    picker = (owner_ref[...] == source).astype(jnp.bfloat16)
    chosen = jnp.dot(picker, branch, preferred_element_type=jnp.float32).astype(jnp.bfloat16)
    relayed = jnp.dot(chosen, proj_ref[...], preferred_element_type=jnp.float32)
    relayed = relayed.astype(jnp.bfloat16).astype(jnp.float32)
    scale = lax.rsqrt(jnp.mean(relayed * relayed, axis=1, keepdims=True) + 1e-06)
    rows_ref[...] = (relayed * scale * gain_ref[...]).astype(jnp.bfloat16)


def relay(parts, proj, owner, gain):
    rows = owner.shape[0]
    features, talk_features = proj.shape
    return pl.pallas_call(
        functools.partial(relay_kernel, len(parts)),
        out_shape=[
            jax.ShapeDtypeStruct((rows, features), jnp.bfloat16),
            jax.ShapeDtypeStruct((rows, talk_features), jnp.bfloat16),
        ],
        in_specs=[VMEM] * (len(parts) + 3),
        out_specs=[VMEM] * 2,
        compiler_params=pltpu.CompilerParams(vmem_limit_bytes=16 << 20),
        cost_estimate=pl.CostEstimate(
            flops=2 * rows * features * talk_features,
            bytes_accessed=2 * features * talk_features,
            transcendentals=0,
        ),
        name="relay",
    )(*parts, proj, owner[:, None], gain[None, :])


def swap(value, bit, count):
    return lax.ppermute(value, "ep", [(i, i ^ bit) for i in range(count)])


def gather_blocks(own, count):
    blocks = {0: own}
    bit = count // 2
    while bit:
        for mask in sorted(blocks):
            blocks[mask | bit] = swap(blocks[mask], bit, count)
        bit //= 2
    return blocks


def add_up(*terms):
    total = terms[0].astype(jnp.float32)
    for term in terms[1:]:
        total = total + term.astype(jnp.float32)
    return total.astype(jnp.bfloat16)


def scatter_sums(blocks, count):
    parts = {mask: [block] for mask, block in blocks.items()}
    bit = 1
    while bit < count:
        for mask in sorted((m for m in parts if m & bit), reverse=True):
            sent = parts.pop(mask)
            parts[mask ^ bit].append(swap(sent[0] if len(sent) == 1 else add_up(*sent), bit, count))
        bit *= 2
    return parts[0]


def by_gathering(
    thinker_rows,
    think_route,
    think_weight,
    think_gate,
    think_up,
    think_down,
    proj_weight,
    owner_map,
    talk_gain,
    talk_route,
    talk_weight,
    talk_gate,
    talk_up,
    talk_down,
):
    count = lax.axis_size("ep")
    expert = lax.axis_index("ep").astype(jnp.int32).reshape(1)
    packed = pack(thinker_rows, think_route, think_weight, talk_route, talk_weight, count)
    gathered = gather_blocks(packed, count)
    done = {}
    for half in range(2):
        masks = list(range(half * count // 2, (half + 1) * count // 2))
        blocks = [gathered[m] for m in masks]
        groups = [[i] for i in range(len(masks))]
        outs = run_expert(
            blocks, blocks, groups, think_gate, think_up, think_down, expert, count, 0, "thinker"
        )
        done.update(zip(masks, outs, strict=True))
    thinker_branch, talk_rows = relay(scatter_sums(done, count), proj_weight, owner_map, talk_gain)
    talk_blocks = gather_blocks(talk_rows, count)
    masks = list(range(count))
    outs = run_expert(
        [talk_blocks[m] for m in masks],
        [gathered[m][:, thinker_rows.shape[1] :] for m in masks],
        [[i] for i in masks],
        talk_gate,
        talk_up,
        talk_down,
        expert,
        count,
        2 * count,
        "talker",
    )
    talker_branch = add_up(*scatter_sums(dict(zip(masks, outs, strict=True)), count))
    return (thinker_branch, talker_branch)


def solution(mesh):
    count = mesh.shape["ep"]
    dense = mesh.shape["sess"] == 1 and count & (count - 1) == 0 and count <= 16
    return jax.shard_map(
        by_gathering if dense else on_device,
        mesh=mesh,
        in_specs=(
            P(("grp", "ep", "sess"), None),
            P(("grp", "ep", "sess"), None),
            P(("grp", "ep", "sess"), None),
            P("ep", None, "sess"),
            P("ep", None, "sess"),
            P("ep", "sess", None),
            P(None, "sess"),
            P(("grp", "ep")),
            P(),
            P(("grp", "ep", "sess"), None),
            P(("grp", "ep", "sess"), None),
            P(("ep", "sess"), None, None),
            P(("ep", "sess"), None, None),
            P(("ep", "sess"), None, None),
        ),
        out_specs=(P(("grp", "ep", "sess"), None), P(("grp", "ep", "sess"), None)),
        check_vma=False,
    )
```

```python
import functools

import jax
import jax.numpy as jnp
from jax import lax
from jax.experimental import pallas as pl
from jax.experimental.pallas import tpu as pltpu
from jax.sharding import PartitionSpec as P


def slot_places(route, experts):
    picks = route.shape[0] * route.shape[1]
    chosen = route.reshape(picks)
    onehot = (chosen[:, None] == jnp.arange(experts, dtype=jnp.int32)[None, :]).astype(jnp.int32)
    before = jnp.cumsum(onehot, axis=0) - onehot
    return (chosen, jnp.sum(before * onehot, axis=1))


def pack_rows(row_block, route, experts, capacity):
    chosen, places = slot_places(route, experts)
    target = chosen * capacity + places
    copies = jnp.repeat(row_block, route.shape[1], axis=0)
    buffer = (
        jnp.zeros((experts * capacity, row_block.shape[1]), jnp.bfloat16).at[target].set(copies)
    )
    return (buffer, target)


def combine_rows(returned, target, weights):
    sessions, picks = weights.shape
    gathered = returned[target].astype(jnp.float32).reshape(sessions, picks, returned.shape[1])
    norm_weights = weights / jnp.sum(weights, axis=1, keepdims=True)
    return jnp.sum(gathered * norm_weights[:, :, None], axis=1).astype(jnp.bfloat16)


def swiglu(slab, gate_m, up_m, down_m):
    gate = jnp.dot(slab, gate_m, preferred_element_type=jnp.float32)
    upper = jnp.dot(slab, up_m, preferred_element_type=jnp.float32)
    hidden = (jax.nn.silu(gate) * upper).astype(jnp.bfloat16)
    return jnp.dot(hidden, down_m, preferred_element_type=jnp.float32)


def on_device(
    thinker_rows,
    think_route,
    think_weight,
    think_gate,
    think_up,
    think_down,
    proj_weight,
    owner_map,
    talk_gain,
    talk_route,
    talk_weight,
    talk_gate,
    talk_up,
    talk_down,
):
    sessions = thinker_rows.shape[0]
    features = thinker_rows.shape[1]
    talk_features = talk_gate.shape[1]
    ep_count = lax.axis_size("ep")
    sess_count = lax.axis_size("sess")
    think_picks = think_route.shape[1]
    think_capacity = min(sessions, max(2, 2 * sessions * think_picks // ep_count))
    buffer, target = pack_rows(thinker_rows, think_route, ep_count, think_capacity)
    buffer = buffer.reshape(ep_count, think_capacity, features)
    gate_half = think_gate[0]
    up_half = think_up[0]
    down_half = think_down[0]
    paired = lax.all_gather(buffer, "sess", axis=1, tiled=True)
    arrived = lax.all_to_all(paired, "ep", split_axis=0, concat_axis=0, tiled=True)
    flattened = arrived.reshape(arrived.shape[0] * arrived.shape[1], features)
    result = swiglu(flattened, gate_half, up_half, down_half)
    partial_value = result.reshape(arrived.shape[0], arrived.shape[1], features)
    summed = lax.psum_scatter(partial_value, "sess", scatter_dimension=1, tiled=True).astype(
        jnp.bfloat16
    )
    returned = lax.all_to_all(summed, "ep", split_axis=0, concat_axis=0, tiled=True).reshape(
        ep_count * think_capacity, features
    )
    thinker_branch = combine_rows(returned, target, think_weight)
    projected = jnp.dot(
        lax.all_gather(thinker_branch, "sess", axis=0, tiled=True),
        proj_weight,
        preferred_element_type=jnp.float32,
    ).astype(jnp.bfloat16)
    block_rows = owner_map.shape[0]
    picker = (owner_map[:, None] == jnp.arange(block_rows, dtype=jnp.int32)[None, :]).astype(
        jnp.bfloat16
    )
    selected = jnp.dot(picker, projected, preferred_element_type=jnp.float32).astype(jnp.bfloat16)
    own_rows = lax.all_to_all(selected, "sess", split_axis=0, concat_axis=1, tiled=True).astype(
        jnp.float32
    )
    scale = lax.rsqrt(jnp.mean(own_rows * own_rows, axis=1, keepdims=True) + 1e-06)
    talk_rows = (own_rows * scale * talk_gain[None, :]).astype(jnp.bfloat16)
    talk_experts = ep_count * sess_count
    talk_picks = talk_route.shape[1]
    talk_capacity = min(sessions, max(2, 2 * sessions * talk_picks // talk_experts))
    talk_buffer, talk_target = pack_rows(talk_rows, talk_route, talk_experts, talk_capacity)
    talk_gate_m = talk_gate[0]
    talk_up_m = talk_up[0]
    talk_down_m = talk_down[0]
    sectioned_in = talk_buffer.reshape(talk_experts, talk_capacity, talk_features)
    portion = lax.all_to_all(sectioned_in, ("ep", "sess"), split_axis=0, concat_axis=0, tiled=True)
    flattened = portion.reshape(portion.shape[0] * portion.shape[1], talk_features)
    result = swiglu(flattened, talk_gate_m, talk_up_m, talk_down_m).astype(jnp.bfloat16)
    finished = result.reshape(portion.shape[0], portion.shape[1], talk_features)
    talk_returned = lax.all_to_all(
        finished, ("ep", "sess"), split_axis=0, concat_axis=0, tiled=True
    )
    talk_returned = talk_returned.reshape(talk_experts * talk_capacity, talk_features)
    talker_branch = combine_rows(talk_returned, talk_target, talk_weight)
    return (thinker_branch, talker_branch)


VMEM = pl.BlockSpec(memory_space=pltpu.VMEM)
HBM = pl.BlockSpec(memory_space=pltpu.HBM)
LANES = 128
WORK_VMEM = 6 << 20
LOAD_1_BESIDE = 10 << 20
LOAD_2_BESIDE = 12 << 20
MOST_VMEM = 63 << 20


def width_of_table(experts):
    return -(-4 * experts // LANES) * LANES


def share_table(lane, route, weights, first, experts):
    shares = weights / jnp.sum(weights, axis=0, keepdims=True)
    table = jnp.zeros(lane.shape, jnp.float32)
    for pick in range(weights.shape[0]):
        expert = route[pick : pick + 1, :] + first
        hit = (lane == expert) | (lane == expert + experts)
        table = table + jnp.where(hit, shares[pick : pick + 1, :], 0.0)
    return table


def pack_kernel(experts, picks, talk_picks, rows_ref, choices_ref, out_ref):
    count, features = rows_ref.shape
    out_ref[:, :features] = rows_ref[...]
    lane = lax.broadcasted_iota(jnp.int32, (out_ref.shape[1] - features, count), 0)
    choices, table, start = choices_ref[...], jnp.zeros(lane.shape, jnp.float32), 0
    for size, first in ((picks, 0), (talk_picks, 2 * experts)):
        route = choices[start : start + size].astype(jnp.int32)
        weights = choices[start + size : start + 2 * size]
        table = table + share_table(lane, route, weights, first, experts)
        start += 2 * size
    high = table.astype(jnp.bfloat16).astype(jnp.float32)
    fine = ((lane >= experts) & (lane < 2 * experts)) | (lane >= 3 * experts)
    both = jnp.where(fine, table - high, high)
    out_ref[:, features:] = both.T.astype(jnp.bfloat16)


def pack(rows, route, weight, talk_route, talk_weight, experts):
    count, features = rows.shape
    given = (route.astype(jnp.float32), weight, talk_route.astype(jnp.float32), talk_weight)
    choices = jnp.concatenate(given, axis=1).T
    return pl.pallas_call(
        functools.partial(pack_kernel, experts, route.shape[1], talk_route.shape[1]),
        out_shape=jax.ShapeDtypeStruct((count, features + width_of_table(experts)), jnp.bfloat16),
        in_specs=[VMEM] * 2,
        out_specs=VMEM,
        compiler_params=pltpu.CompilerParams(vmem_limit_bytes=WORK_VMEM),
        cost_estimate=pl.CostEstimate(flops=1 << 20, bytes_accessed=1 << 18, transcendentals=0),
        name="pack",
    )(rows, choices)


PIECES = 4


def start_copies(sources, targets, sems):
    copies = []
    for source, target in zip(sources, targets, strict=True):
        step = source.shape[-2] // PIECES
        for piece in range(PIECES):
            cut = pl.ds(piece * step, step)
            place = (*(slice(None),) * (len(source.shape) - 2), cut)
            copies.append(
                pltpu.make_async_copy(source.at[place], target.at[place], sems.at[len(copies)])
            )
    for copy in copies:
        copy.start()
    return copies


def fetch_kernel(count, *refs):
    for copy in start_copies(refs[:count], refs[count : 2 * count], refs[-1]):
        copy.wait()


def bytes_of(*arrays):
    return sum(a.size * a.dtype.itemsize for a in arrays)


def fetch(arrays, beside):
    return pl.pallas_call(
        functools.partial(fetch_kernel, len(arrays)),
        out_shape=[jax.ShapeDtypeStruct(a.shape, a.dtype) for a in arrays],
        in_specs=[HBM] * len(arrays),
        out_specs=[VMEM] * len(arrays),
        scratch_shapes=[pltpu.SemaphoreType.DMA((len(arrays) * PIECES,))],
        compiler_params=pltpu.CompilerParams(
            vmem_limit_bytes=MOST_VMEM - beside - bytes_of(*arrays)
        ),
        cost_estimate=pl.CostEstimate(
            flops=1 << 20, bytes_accessed=2 * bytes_of(*arrays), transcendentals=0
        ),
        name="fetch",
    )(*arrays)


def share_of(columns, first, experts, expert):
    lane = lax.broadcasted_iota(jnp.int32, columns.shape, 1)
    hit = (lane == first + expert) | (lane == first + experts + expert)
    return jnp.sum(jnp.where(hit, columns.astype(jnp.float32), 0.0), axis=1, keepdims=True)


def tile_of(width, most):
    tile = min(width, most)
    while width % tile:
        tile -= LANES
    return tile


def expert_kernel(plan, *refs):
    blocks, wanted, tables, wanted_tables, rows, groups, experts, first, pair = plan
    sources, refs = refs[:blocks], refs[blocks:]
    table_sources, refs = refs[:tables], refs[tables:]
    weights, refs = refs[: 3 * len(pair)], refs[3 * len(pair) :]
    outs, refs = refs[: len(groups)], refs[len(groups) :]
    if not tables:
        table_ref, refs = refs[0], refs[1:]
    slab_ref, *hidden_refs = refs
    features, hidden_units = slab_ref.shape[1], weights[0].shape[-1]
    columns = []
    for index, (block, place) in enumerate(wanted):
        source = slice(place * rows, (place + 1) * rows)
        target = slice(index * rows, (index + 1) * rows)
        slab_ref[target, :] = sources[block][source, :features]
        if tables:
            table, place = wanted_tables[index]
            columns.append(table_sources[table][place * rows : (place + 1) * rows, :])
        else:
            table_ref[target, :] = sources[block][source, features:]
            columns.append(sources[block][source, features:])
    columns = jnp.concatenate(columns, axis=0)
    slab = slab_ref[...]
    step = tile_of(hidden_units, 256)
    for number, offset in enumerate(pair):
        gate_ref, up_ref = weights[3 * number : 3 * number + 2]
        share = share_of(columns, first, experts, lax.axis_index("ep") ^ offset)
        for start in range(0, hidden_units, step):
            cut = slice(start, start + step)
            gate = jnp.dot(slab, gate_ref[0, :, cut], preferred_element_type=jnp.float32)
            upper = jnp.dot(slab, up_ref[0, :, cut], preferred_element_type=jnp.float32)
            hidden = gate / (1.0 + jnp.exp(-gate)) * upper
            hidden_refs[number][:, cut] = (hidden * share).astype(jnp.bfloat16)
    step = tile_of(features, 512)
    for start in range(0, features, step):
        cut = slice(start, start + step)
        value = 0.0
        for number in range(len(pair)):
            down = weights[3 * number + 2][0, :, cut]
            value += jnp.dot(hidden_refs[number][...], down, preferred_element_type=jnp.float32)
        value = value.astype(jnp.bfloat16)
        for out, group in zip(outs, groups, strict=True):
            for place, index in enumerate(group):
                out[place * rows : (place + 1) * rows, cut] = value[index * rows : (index + 1) * rows]


def distinct(placed):
    arrays = list({id(array): array for array, _ in placed}.values())
    index = {id(array): i for i, array in enumerate(arrays)}
    return arrays, tuple((index[id(array)], place) for array, place in placed)


def run_expert(blocks, rows, tables, groups, weights, experts, first):
    arrays, wanted = distinct(blocks)
    table_arrays, wanted_tables = distinct(tables or [])
    total = len(blocks) * rows
    _, features, hidden_units = weights[0][1].shape
    shapes = [jax.ShapeDtypeStruct((len(g) * rows, features), jnp.bfloat16) for g in groups]
    if not tables:
        shapes.append(jax.ShapeDtypeStruct((total, arrays[0].shape[1] - features), jnp.bfloat16))
    pair = tuple(w[0] for w in weights)
    plan = (len(arrays), wanted, len(table_arrays), wanted_tables, rows, groups, experts, first, pair)
    given = [*arrays, *table_arrays, *(a for w in weights for a in w[1:])]
    return pl.pallas_call(
        functools.partial(expert_kernel, plan),
        out_shape=shapes,
        in_specs=[VMEM] * len(given),
        out_specs=[VMEM] * len(shapes),
        scratch_shapes=[
            pltpu.VMEM((total, features), jnp.bfloat16),
            *(pltpu.VMEM((total, hidden_units), jnp.bfloat16) for _ in pair),
        ],
        compiler_params=pltpu.CompilerParams(
            vmem_limit_bytes=WORK_VMEM + 2 * total * (features + len(pair) * hidden_units)
        ),
        cost_estimate=pl.CostEstimate(
            flops=6 * len(pair) * total * features * hidden_units,
            bytes_accessed=6 * len(pair) * features * hidden_units,
            transcendentals=len(pair) * total * hidden_units,
        ),
    )(*given)


def total_of(refs, places, rows):
    terms = [
        ref[place * rows : (place + 1) * rows, :].astype(jnp.float32)
        for ref, place in zip(refs, places, strict=True)
    ]
    total = terms[0]
    for term in terms[1:]:
        total = total + term
    return total.astype(jnp.bfloat16)


def sum_kernel(plans, rows, *refs):
    for index, plan in enumerate(plans):
        places = [place for _, place in plan]
        total = total_of([refs[i] for i, _ in plan], places, rows)
        refs[-1][index * rows : (index + 1) * rows, :] = total


def add_up(*sums, rows):
    arrays, index = distinct([pair for terms in sums for pair in terms])
    plans = []
    for terms in sums:
        plans.append(index[: len(terms)])
        index = index[len(terms) :]
    features = arrays[0].shape[1]
    return pl.pallas_call(
        functools.partial(sum_kernel, tuple(plans), rows),
        out_shape=jax.ShapeDtypeStruct((len(sums) * rows, features), jnp.bfloat16),
        in_specs=[VMEM] * len(arrays),
        out_specs=VMEM,
        compiler_params=pltpu.CompilerParams(vmem_limit_bytes=WORK_VMEM),
        cost_estimate=pl.CostEstimate(
            flops=len(arrays) * rows * features, bytes_accessed=1 << 16, transcendentals=0
        ),
        name="add_up",
    )(*arrays)


def relay_kernel(places, *refs):
    parts, refs = refs[: len(places)], refs[len(places) :]
    proj_ref, owner_ref, gain_ref, branch_ref, rows_ref = refs
    rows = branch_ref.shape[0]
    branch = total_of(parts, places, rows)
    branch_ref[...] = branch
    source = lax.broadcasted_iota(jnp.int32, (rows, rows), 0)
    picker = jnp.where(source == owner_ref[...], 1.0, 0.0).T.astype(jnp.bfloat16)
    chosen = jnp.dot(picker, branch, preferred_element_type=jnp.float32).astype(jnp.bfloat16)
    relayed = jnp.dot(chosen, proj_ref[...], preferred_element_type=jnp.float32)
    relayed = relayed.astype(jnp.bfloat16).astype(jnp.float32)
    scale = lax.rsqrt(jnp.mean(relayed * relayed, axis=1, keepdims=True) + 1e-06)
    rows_ref[...] = (relayed * scale * gain_ref[...]).astype(jnp.bfloat16)


def relay(parts, proj, owner, gain):
    rows = owner.shape[0]
    arrays, places = zip(*parts, strict=True)
    features, talk_features = proj.shape
    return pl.pallas_call(
        functools.partial(relay_kernel, places),
        out_shape=[
            jax.ShapeDtypeStruct((rows, features), jnp.bfloat16),
            jax.ShapeDtypeStruct((rows, talk_features), jnp.bfloat16),
        ],
        in_specs=[VMEM] * (len(arrays) + 3),
        out_specs=[VMEM] * 2,
        compiler_params=pltpu.CompilerParams(vmem_limit_bytes=WORK_VMEM),
        cost_estimate=pl.CostEstimate(
            flops=2 * rows * features * talk_features,
            bytes_accessed=2 * features * talk_features,
            transcendentals=0,
        ),
        name="relay",
    )(*arrays, proj, owner[None, :], gain[None, :])


def low_bit(mask):
    return mask & -mask


def swap(value, bit, count):
    return lax.ppermute(value, "ep", [(i, i ^ bit) for i in range(count)])


def chips_crossed(mask):
    return (mask >> 1).bit_count()


def calls(masks, top):
    late = [m for m in masks if m & 2 and m & top]
    early = [m for m in masks if chips_crossed(m) <= 1]
    middle = [m for m in masks if m not in late and m not in early]
    return {"early": early, "middle": middle, "late": late}


def gather_blocks(own, count, step):
    blocks = {0: own}
    for mask in sorted(range(step, count, step), key=int.bit_count):
        low = low_bit(mask)
        blocks[mask] = swap(blocks[mask - low], low, count)
    return blocks


def expert_sums(blocks, rows, tables, weights, count, first):
    parts, given = {}, {}
    for masks in calls(sorted(blocks), count // 2).values():
        odd = tuple(m for m in reversed(masks) if m & 1)
        groups = tuple((m,) for m in masks if not m & 1) + ((odd,) if odd else ())
        outs = run_expert(
            [(blocks[m], 0) for m in masks],
            rows,
            tables and [tables[m] for m in masks],
            tuple(tuple(masks.index(m) for m in g) for g in groups),
            weights,
            count,
            first,
        )
        given.update({m: (outs[-1], place) for place, m in enumerate(masks)})
        for group, out in zip(groups, outs, strict=False):
            if group != odd:
                parts[group[0]] = [(out, 0)]
        if odd:
            crossing = swap(outs[len(groups) - 1], 1, count)
            for place, m in enumerate(odd):
                parts[m ^ 1].append((crossing, place))
    bit = 2
    while bit < count:
        for m in sorted((m for m in parts if m & bit), reverse=True):
            terms = parts.pop(m)
            sent = terms[0][0] if len(terms) == 1 else add_up(terms, rows=rows)
            parts[m ^ bit].append((swap(sent, bit, count), 0))
        bit *= 2
    return parts[0], given


def by_gathering(
    thinker_rows,
    think_route,
    think_weight,
    think_gate,
    think_up,
    think_down,
    proj_weight,
    owner_map,
    talk_gain,
    talk_route,
    talk_weight,
    talk_gate,
    talk_up,
    talk_down,
):
    count = lax.axis_size("ep")
    own = pack(thinker_rows, think_route, think_weight, talk_route, talk_weight, count)
    arrays = (think_gate, think_up, think_down)
    weights = fetch(arrays, LOAD_1_BESIDE)
    (proj,) = fetch((proj_weight,), LOAD_2_BESIDE)
    blocks, rows = gather_blocks(own, count, 1), own.shape[0]
    parts, tables = expert_sums(blocks, rows, None, [(0, *weights)], count, 0)
    thinker_branch, talk_rows = relay(parts, proj, owner_map, talk_gain)
    arrays = (talk_gate, talk_up, talk_down)
    other = [swap(a, 1, count) for a in arrays]
    blocks = gather_blocks(talk_rows, count, 2)
    weights = [(0, *arrays), (1, *other)]
    parts, _ = expert_sums(blocks, rows, tables, weights, count, 2 * count)
    return (thinker_branch, add_up(parts, rows=rows))


def solution(mesh):
    count = mesh.shape["ep"]
    dense = mesh.shape["sess"] == 1 and count == 16
    return jax.shard_map(
        by_gathering if dense else on_device,
        mesh=mesh,
        in_specs=(
            P(("grp", "ep", "sess"), None),
            P(("grp", "ep", "sess"), None),
            P(("grp", "ep", "sess"), None),
            P("ep", None, "sess"),
            P("ep", None, "sess"),
            P("ep", "sess", None),
            P(None, "sess"),
            P(("grp", "ep")),
            P(),
            P(("grp", "ep", "sess"), None),
            P(("grp", "ep", "sess"), None),
            P(("ep", "sess"), None, None),
            P(("ep", "sess"), None, None),
            P(("ep", "sess"), None, None),
        ),
        out_specs=(P(("grp", "ep", "sess"), None), P(("grp", "ep", "sess"), None)),
        check_vma=False,
    )
```

```python
import functools

import jax
import jax.numpy as jnp
from jax import lax
from jax.experimental import pallas as pl
from jax.experimental.pallas import tpu as pltpu
from jax.sharding import PartitionSpec as P


def slot_places(route, experts):
    picks = route.shape[0] * route.shape[1]
    chosen = route.reshape(picks)
    onehot = (chosen[:, None] == jnp.arange(experts, dtype=jnp.int32)[None, :]).astype(jnp.int32)
    before = jnp.cumsum(onehot, axis=0) - onehot
    return (chosen, jnp.sum(before * onehot, axis=1))


def pack_rows(row_block, route, experts, capacity):
    chosen, places = slot_places(route, experts)
    target = chosen * capacity + places
    copies = jnp.repeat(row_block, route.shape[1], axis=0)
    buffer = (
        jnp.zeros((experts * capacity, row_block.shape[1]), jnp.bfloat16).at[target].set(copies)
    )
    return (buffer, target)


def combine_rows(returned, target, weights):
    sessions, picks = weights.shape
    gathered = returned[target].astype(jnp.float32).reshape(sessions, picks, returned.shape[1])
    norm_weights = weights / jnp.sum(weights, axis=1, keepdims=True)
    return jnp.sum(gathered * norm_weights[:, :, None], axis=1).astype(jnp.bfloat16)


def swiglu(slab, gate_m, up_m, down_m):
    gate = jnp.dot(slab, gate_m, preferred_element_type=jnp.float32)
    upper = jnp.dot(slab, up_m, preferred_element_type=jnp.float32)
    hidden = (jax.nn.silu(gate) * upper).astype(jnp.bfloat16)
    return jnp.dot(hidden, down_m, preferred_element_type=jnp.float32)


def on_device(
    thinker_rows,
    think_route,
    think_weight,
    think_gate,
    think_up,
    think_down,
    proj_weight,
    owner_map,
    talk_gain,
    talk_route,
    talk_weight,
    talk_gate,
    talk_up,
    talk_down,
):
    sessions = thinker_rows.shape[0]
    features = thinker_rows.shape[1]
    talk_features = talk_gate.shape[1]
    ep_count = lax.axis_size("ep")
    sess_count = lax.axis_size("sess")
    think_picks = think_route.shape[1]
    think_capacity = min(sessions, max(2, 2 * sessions * think_picks // ep_count))
    buffer, target = pack_rows(thinker_rows, think_route, ep_count, think_capacity)
    buffer = buffer.reshape(ep_count, think_capacity, features)
    gate_half = think_gate[0]
    up_half = think_up[0]
    down_half = think_down[0]
    paired = lax.all_gather(buffer, "sess", axis=1, tiled=True)
    arrived = lax.all_to_all(paired, "ep", split_axis=0, concat_axis=0, tiled=True)
    flattened = arrived.reshape(arrived.shape[0] * arrived.shape[1], features)
    result = swiglu(flattened, gate_half, up_half, down_half)
    partial_value = result.reshape(arrived.shape[0], arrived.shape[1], features)
    summed = lax.psum_scatter(partial_value, "sess", scatter_dimension=1, tiled=True).astype(
        jnp.bfloat16
    )
    returned = lax.all_to_all(summed, "ep", split_axis=0, concat_axis=0, tiled=True).reshape(
        ep_count * think_capacity, features
    )
    thinker_branch = combine_rows(returned, target, think_weight)
    projected = jnp.dot(
        lax.all_gather(thinker_branch, "sess", axis=0, tiled=True),
        proj_weight,
        preferred_element_type=jnp.float32,
    ).astype(jnp.bfloat16)
    block_rows = owner_map.shape[0]
    picker = (owner_map[:, None] == jnp.arange(block_rows, dtype=jnp.int32)[None, :]).astype(
        jnp.bfloat16
    )
    selected = jnp.dot(picker, projected, preferred_element_type=jnp.float32).astype(jnp.bfloat16)
    own_rows = lax.all_to_all(selected, "sess", split_axis=0, concat_axis=1, tiled=True).astype(
        jnp.float32
    )
    scale = lax.rsqrt(jnp.mean(own_rows * own_rows, axis=1, keepdims=True) + 1e-06)
    talk_rows = (own_rows * scale * talk_gain[None, :]).astype(jnp.bfloat16)
    talk_experts = ep_count * sess_count
    talk_picks = talk_route.shape[1]
    talk_capacity = min(sessions, max(2, 2 * sessions * talk_picks // talk_experts))
    talk_buffer, talk_target = pack_rows(talk_rows, talk_route, talk_experts, talk_capacity)
    talk_gate_m = talk_gate[0]
    talk_up_m = talk_up[0]
    talk_down_m = talk_down[0]
    sectioned_in = talk_buffer.reshape(talk_experts, talk_capacity, talk_features)
    portion = lax.all_to_all(sectioned_in, ("ep", "sess"), split_axis=0, concat_axis=0, tiled=True)
    flattened = portion.reshape(portion.shape[0] * portion.shape[1], talk_features)
    result = swiglu(flattened, talk_gate_m, talk_up_m, talk_down_m).astype(jnp.bfloat16)
    finished = result.reshape(portion.shape[0], portion.shape[1], talk_features)
    talk_returned = lax.all_to_all(
        finished, ("ep", "sess"), split_axis=0, concat_axis=0, tiled=True
    )
    talk_returned = talk_returned.reshape(talk_experts * talk_capacity, talk_features)
    talker_branch = combine_rows(talk_returned, talk_target, talk_weight)
    return (thinker_branch, talker_branch)


VMEM = pl.BlockSpec(memory_space=pltpu.VMEM)
HBM = pl.BlockSpec(memory_space=pltpu.HBM)
LANES = 128
WORK_VMEM = 6 << 20
LOAD_1_BESIDE = 10 << 20
LOAD_2_BESIDE = 12 << 20
MOST_VMEM = 63 << 20


def width_of_table(experts):
    return -(-4 * experts // LANES) * LANES


def share_table(lane, route, weights, first, experts):
    shares = weights / jnp.sum(weights, axis=0, keepdims=True)
    table = jnp.zeros(lane.shape, jnp.float32)
    for pick in range(weights.shape[0]):
        expert = route[pick : pick + 1, :] + first
        hit = (lane == expert) | (lane == expert + experts)
        table = table + jnp.where(hit, shares[pick : pick + 1, :], 0.0)
    return table


def pack_kernel(experts, picks, talk_picks, rows_ref, choices_ref, out_ref):
    count, features = rows_ref.shape
    out_ref[:, :features] = rows_ref[...]
    lane = lax.broadcasted_iota(jnp.int32, (out_ref.shape[1] - features, count), 0)
    choices, table, start = choices_ref[...], jnp.zeros(lane.shape, jnp.float32), 0
    for size, first in ((picks, 0), (talk_picks, 2 * experts)):
        route = choices[start : start + size].astype(jnp.int32)
        weights = choices[start + size : start + 2 * size]
        table = table + share_table(lane, route, weights, first, experts)
        start += 2 * size
    high = table.astype(jnp.bfloat16).astype(jnp.float32)
    fine = ((lane >= experts) & (lane < 2 * experts)) | (lane >= 3 * experts)
    both = jnp.where(fine, table - high, high)
    out_ref[:, features:] = both.T.astype(jnp.bfloat16)


def pack(rows, route, weight, talk_route, talk_weight, experts):
    count, features = rows.shape
    given = (route.astype(jnp.float32), weight, talk_route.astype(jnp.float32), talk_weight)
    choices = jnp.concatenate(given, axis=1).T
    return pl.pallas_call(
        functools.partial(pack_kernel, experts, route.shape[1], talk_route.shape[1]),
        out_shape=jax.ShapeDtypeStruct((count, features + width_of_table(experts)), jnp.bfloat16),
        in_specs=[VMEM] * 2,
        out_specs=VMEM,
        compiler_params=pltpu.CompilerParams(vmem_limit_bytes=WORK_VMEM),
        cost_estimate=pl.CostEstimate(flops=1 << 20, bytes_accessed=1 << 18, transcendentals=0),
        name="pack",
    )(rows, choices)


PIECES = 4


def start_copies(sources, targets, sems):
    copies = []
    for source, target in zip(sources, targets, strict=True):
        step = source.shape[-2] // PIECES
        for piece in range(PIECES):
            cut = pl.ds(piece * step, step)
            place = (*(slice(None),) * (len(source.shape) - 2), cut)
            copies.append(
                pltpu.make_async_copy(source.at[place], target.at[place], sems.at[len(copies)])
            )
    for copy in copies:
        copy.start()
    return copies


def fetch_kernel(count, *refs):
    for copy in start_copies(refs[:count], refs[count : 2 * count], refs[-1]):
        copy.wait()


def bytes_of(*arrays):
    return sum(a.size * a.dtype.itemsize for a in arrays)


def fetch(arrays, beside):
    return pl.pallas_call(
        functools.partial(fetch_kernel, len(arrays)),
        out_shape=[jax.ShapeDtypeStruct(a.shape, a.dtype) for a in arrays],
        in_specs=[HBM] * len(arrays),
        out_specs=[VMEM] * len(arrays),
        scratch_shapes=[pltpu.SemaphoreType.DMA((len(arrays) * PIECES,))],
        compiler_params=pltpu.CompilerParams(
            vmem_limit_bytes=MOST_VMEM - beside - bytes_of(*arrays)
        ),
        cost_estimate=pl.CostEstimate(
            flops=1 << 20, bytes_accessed=2 * bytes_of(*arrays), transcendentals=0
        ),
        name="fetch",
    )(*arrays)


def share_of(columns, first, experts, expert):
    lane = lax.broadcasted_iota(jnp.int32, columns.shape, 1)
    hit = (lane == first + expert) | (lane == first + experts + expert)
    return jnp.sum(jnp.where(hit, columns.astype(jnp.float32), 0.0), axis=1, keepdims=True)


def tile_of(width, most):
    tile = min(width, most)
    while width % tile:
        tile -= LANES
    return tile


def expert_kernel(plan, *refs):
    blocks, wanted, tables, wanted_tables, rows, groups, experts, first, pair = plan
    sources, refs = refs[:blocks], refs[blocks:]
    table_sources, refs = refs[:tables], refs[tables:]
    weights, refs = refs[: 3 * len(pair)], refs[3 * len(pair) :]
    outs, refs = refs[: len(groups)], refs[len(groups) :]
    if not tables:
        table_ref, refs = refs[0], refs[1:]
    slab_ref, *hidden_refs = refs
    features, hidden_units = slab_ref.shape[1], weights[0].shape[-1]
    columns = []
    for index, (block, place) in enumerate(wanted):
        source = slice(place * rows, (place + 1) * rows)
        target = slice(index * rows, (index + 1) * rows)
        slab_ref[target, :] = sources[block][source, :features]
        if tables:
            table, place = wanted_tables[index]
            columns.append(table_sources[table][place * rows : (place + 1) * rows, :])
        else:
            table_ref[target, :] = sources[block][source, features:]
            columns.append(sources[block][source, features:])
    spare = slab_ref.shape[0] - len(wanted) * rows
    for start in range(slab_ref.shape[0] - spare, slab_ref.shape[0], rows):
        slab_ref[start : start + rows, :] = slab_ref[:rows, :]
        columns.append(columns[0])
    columns = jnp.concatenate(columns, axis=0)
    slab = slab_ref[...]
    step = tile_of(hidden_units, 256)
    for number, offset in enumerate(pair):
        gate_ref, up_ref = weights[3 * number : 3 * number + 2]
        share = share_of(columns, first, experts, lax.axis_index("ep") ^ offset)
        for start in range(0, hidden_units, step):
            cut = slice(start, start + step)
            gate = jnp.dot(slab, gate_ref[0, :, cut], preferred_element_type=jnp.float32)
            upper = jnp.dot(slab, up_ref[0, :, cut], preferred_element_type=jnp.float32)
            hidden = gate / (1.0 + jnp.exp(-gate)) * upper
            hidden_refs[number][:, cut] = (hidden * share).astype(jnp.bfloat16)
    step = tile_of(features, 512)
    for start in range(0, features, step):
        cut = slice(start, start + step)
        value = 0.0
        for number in range(len(pair)):
            down = weights[3 * number + 2][0, :, cut]
            value += jnp.dot(hidden_refs[number][...], down, preferred_element_type=jnp.float32)
        value = value.astype(jnp.bfloat16)
        for out, group in zip(outs, groups, strict=True):
            for place, index in enumerate(group):
                out[place * rows : (place + 1) * rows, cut] = value[index * rows : (index + 1) * rows]


def distinct(placed):
    arrays = list({id(array): array for array, _ in placed}.values())
    index = {id(array): i for i, array in enumerate(arrays)}
    return arrays, tuple((index[id(array)], place) for array, place in placed)


def run_expert(blocks, rows, tables, groups, weights, experts, first):
    arrays, wanted = distinct(blocks)
    table_arrays, wanted_tables = distinct(tables or [])
    total = len(blocks) * rows
    padded = max(total, LANES) if total * 2 >= LANES else total
    _, features, hidden_units = weights[0][1].shape
    shapes = [jax.ShapeDtypeStruct((len(g) * rows, features), jnp.bfloat16) for g in groups]
    if not tables:
        shapes.append(jax.ShapeDtypeStruct((total, arrays[0].shape[1] - features), jnp.bfloat16))
    pair = tuple(w[0] for w in weights)
    plan = (len(arrays), wanted, len(table_arrays), wanted_tables, rows, groups, experts, first, pair)
    given = [*arrays, *table_arrays, *(a for w in weights for a in w[1:])]
    return pl.pallas_call(
        functools.partial(expert_kernel, plan),
        out_shape=shapes,
        in_specs=[VMEM] * len(given),
        out_specs=[VMEM] * len(shapes),
        scratch_shapes=[
            pltpu.VMEM((padded, features), jnp.bfloat16),
            *(pltpu.VMEM((padded, hidden_units), jnp.bfloat16) for _ in pair),
        ],
        compiler_params=pltpu.CompilerParams(
            vmem_limit_bytes=WORK_VMEM + 2 * total * (features + len(pair) * hidden_units)
        ),
        cost_estimate=pl.CostEstimate(
            flops=6 * len(pair) * total * features * hidden_units,
            bytes_accessed=6 * len(pair) * features * hidden_units,
            transcendentals=len(pair) * total * hidden_units,
        ),
    )(*given)


def total_of(refs, places, rows):
    terms = [
        ref[place * rows : (place + 1) * rows, :].astype(jnp.float32)
        for ref, place in zip(refs, places, strict=True)
    ]
    total = terms[0]
    for term in terms[1:]:
        total = total + term
    return total.astype(jnp.bfloat16)


def sum_kernel(plans, rows, *refs):
    for index, plan in enumerate(plans):
        places = [place for _, place in plan]
        total = total_of([refs[i] for i, _ in plan], places, rows)
        refs[-1][index * rows : (index + 1) * rows, :] = total


def add_up(*sums, rows):
    arrays, index = distinct([pair for terms in sums for pair in terms])
    plans = []
    for terms in sums:
        plans.append(index[: len(terms)])
        index = index[len(terms) :]
    features = arrays[0].shape[1]
    return pl.pallas_call(
        functools.partial(sum_kernel, tuple(plans), rows),
        out_shape=jax.ShapeDtypeStruct((len(sums) * rows, features), jnp.bfloat16),
        in_specs=[VMEM] * len(arrays),
        out_specs=VMEM,
        compiler_params=pltpu.CompilerParams(vmem_limit_bytes=WORK_VMEM),
        cost_estimate=pl.CostEstimate(
            flops=len(arrays) * rows * features, bytes_accessed=1 << 16, transcendentals=0
        ),
        name="add_up",
    )(*arrays)


def relay_kernel(places, *refs):
    parts, refs = refs[: len(places)], refs[len(places) :]
    proj_ref, owner_ref, gain_ref, branch_ref, rows_ref = refs
    rows = branch_ref.shape[0]
    branch = total_of(parts, places, rows)
    branch_ref[...] = branch
    source = lax.broadcasted_iota(jnp.int32, (rows, rows), 0)
    picker = jnp.where(source == owner_ref[...], 1.0, 0.0).T.astype(jnp.bfloat16)
    chosen = jnp.dot(picker, branch, preferred_element_type=jnp.float32).astype(jnp.bfloat16)
    relayed = jnp.dot(chosen, proj_ref[...], preferred_element_type=jnp.float32)
    relayed = relayed.astype(jnp.bfloat16).astype(jnp.float32)
    scale = lax.rsqrt(jnp.mean(relayed * relayed, axis=1, keepdims=True) + 1e-06)
    rows_ref[...] = (relayed * scale * gain_ref[...]).astype(jnp.bfloat16)


def relay(parts, proj, owner, gain):
    rows = owner.shape[0]
    arrays, places = zip(*parts, strict=True)
    features, talk_features = proj.shape
    return pl.pallas_call(
        functools.partial(relay_kernel, places),
        out_shape=[
            jax.ShapeDtypeStruct((rows, features), jnp.bfloat16),
            jax.ShapeDtypeStruct((rows, talk_features), jnp.bfloat16),
        ],
        in_specs=[VMEM] * (len(arrays) + 3),
        out_specs=[VMEM] * 2,
        compiler_params=pltpu.CompilerParams(vmem_limit_bytes=WORK_VMEM),
        cost_estimate=pl.CostEstimate(
            flops=2 * rows * features * talk_features,
            bytes_accessed=2 * features * talk_features,
            transcendentals=0,
        ),
        name="relay",
    )(*arrays, proj, owner[None, :], gain[None, :])


def swap(value, bit, count):
    return lax.ppermute(value, "ep", [(i, i ^ bit) for i in range(count)])


def last_step(mask):
    return mask & 1 or mask & 2 or mask


def steps(mask):
    return (mask & 1) + (mask >> 1 & 1) + (mask > 3)


def calls(masks, top):
    late = [m for m in masks if m & 2 and m >= top + top // 2]
    early = [m for m in masks if m < 4 or not m & 2 and m < top + top // 2]
    middle = [m for m in masks if m not in late and m not in early]
    return {"early": early, "middle": middle, "late": late}


def gather_blocks(own, count, step):
    blocks = {0: own}
    for mask in sorted(range(step, count, step), key=steps):
        last = last_step(mask)
        blocks[mask] = swap(blocks[mask - last], last, count)
    return blocks


def expert_sums(blocks, rows, tables, weights, count, first, near=()):
    parts, given = {}, {}
    for masks in calls(sorted(blocks), count // 2).values():
        odd = tuple(m for m in reversed(masks) if m & 1)
        groups = tuple((m,) for m in masks if not m & 1) + ((odd,) if odd else ())
        outs = run_expert(
            [(blocks[m], 0) for m in masks],
            rows,
            tables and [tables[m] for m in masks],
            tuple(tuple(masks.index(m) for m in g) for g in groups),
            weights,
            count,
            first,
        )
        given.update({m: (outs[-1], place) for place, m in enumerate(masks)})
        for group, out in zip(groups, outs, strict=False):
            if group != odd:
                parts[group[0]] = [(out, 0)]
        if odd:
            crossing = swap(outs[len(groups) - 1], 1, count)
            for place, m in enumerate(odd):
                parts[m ^ 1].append((crossing, place))

    def send(masks):
        terms = [parts.pop(m) for m in masks]
        alone = len(terms) == 1 and len(terms[0]) == 1
        sent = terms[0][0][0] if alone else add_up(*terms, rows=rows)
        last = last_step(masks[0])
        came = swap(sent, last, count)
        for place, m in enumerate(masks):
            parts[m - last].append((came, place))

    soon = [m for m in sorted(parts) if m & 2 and m in near]
    if soon:
        send(soon)
    for m in sorted((m for m in parts if m), key=lambda m: (-steps(m), m)):
        send([m])
    return parts[0], given


def by_gathering(
    thinker_rows,
    think_route,
    think_weight,
    think_gate,
    think_up,
    think_down,
    proj_weight,
    owner_map,
    talk_gain,
    talk_route,
    talk_weight,
    talk_gate,
    talk_up,
    talk_down,
):
    count = lax.axis_size("ep")
    own = pack(thinker_rows, think_route, think_weight, talk_route, talk_weight, count)
    arrays = (think_gate, think_up, think_down)
    weights = fetch(arrays[:1], LOAD_1_BESIDE)
    weights += fetch(arrays[1:], LOAD_1_BESIDE + bytes_of(*arrays[:1]))
    (proj,) = fetch((proj_weight,), LOAD_2_BESIDE)
    blocks, rows = gather_blocks(own, count, 1), own.shape[0]
    parts, tables = expert_sums(blocks, rows, None, [(0, *weights)], count, 0)
    thinker_branch, talk_rows = relay(parts, proj, owner_map, talk_gain)
    arrays = (talk_gate, talk_up, talk_down)
    other = [swap(a, 1, count) for a in arrays]
    blocks = gather_blocks(talk_rows, count, 2)
    weights = [(0, *arrays), (1, *other)]
    parts, _ = expert_sums(blocks, rows, tables, weights, count, 2 * count, (2, 6))
    return (thinker_branch, add_up(parts, rows=rows))


def solution(mesh):
    count = mesh.shape["ep"]
    dense = mesh.shape["sess"] == 1 and count == 16
    return jax.shard_map(
        by_gathering if dense else on_device,
        mesh=mesh,
        in_specs=(
            P(("grp", "ep", "sess"), None),
            P(("grp", "ep", "sess"), None),
            P(("grp", "ep", "sess"), None),
            P("ep", None, "sess"),
            P("ep", None, "sess"),
            P("ep", "sess", None),
            P(None, "sess"),
            P(("grp", "ep")),
            P(),
            P(("grp", "ep", "sess"), None),
            P(("grp", "ep", "sess"), None),
            P(("ep", "sess"), None, None),
            P(("ep", "sess"), None, None),
            P(("ep", "sess"), None, None),
        ),
        out_specs=(P(("grp", "ep", "sess"), None), P(("grp", "ep", "sess"), None)),
        check_vma=False,
    )
```
